32 devices in a mesh: row: 4 (over y, x), col: 8 (over z, core).
Axes of the slice: x: 2, y: 2, z: 4, core: 2. Of those that a mesh axis runs over, the one named last changes fastest.
Arguments:
- arrival: float32 [64, 4096], P(None, 'col'), may hold values from 0 to 4
- delay: bfloat16 [4, 4096, 4096], P(None, 'col', 'row'), may hold values from -40 to 20
- occupancy: int32 [4, 8, 8], replicated, may hold values from 0 to 1, as said below
Outputs:
- final_arrival: float32 [64, 4096], P(None, 'col')
- worst: float32 [64], replicated
The draws below stay inside these ranges and needn't reach their ends.
Inputs may be any that keep to these rules, and one draw needn't show every extreme that they name: In every level every column of tiles holds at least one tile with occupancy 1.
All inputs are finite; a program needn't handle non-finite values.
Results may differ from the reference program's by a relative error of at most 0.0009.
Values sent between devices are 32-bit elements; how exact they have to be, the bound alone decides.
A program may use at most 64 MiB of HBM per device.

```python
import jax
import jax.numpy as jnp
from jax import lax

TILE = 512
SCEN = 64
LEVELS = 4
TILES = 8
PINS = 4096


def draw_occupancy(key, part):
    first, second = jax.random.split(jax.random.fold_in(key, 7))
    base = jax.random.randint(first, (LEVELS, TILES, TILES), 0, 2, dtype=jnp.int32)
    picked = jax.random.randint(second, (LEVELS, 1, TILES), 0, TILES, dtype=jnp.int32)
    places = jnp.arange(TILES, dtype=jnp.int32)[None, :, None]
    forced = (places == picked).astype(jnp.int32)
    return jnp.maximum(base, forced)


def draw_delay(key, part):
    spread = jnp.float32(2.5)
    nominal = spread * jnp.sqrt(2.0 * jnp.log(jnp.float32(0.5 * PINS)))
    first, second, third = jax.random.split(jax.random.fold_in(key, 11), 3)
    normal_part = jnp.clip(jax.random.normal(first, (LEVELS, PINS, PINS), jnp.float32), -6.0, 6.0)
    values = spread * normal_part - nominal
    return jnp.clip(values, -40.0, 20.0).astype(jnp.bfloat16)


def levels(rng, shape, pieces, smallest, high):
    level, own = 1.0, jax.random.fold_in(rng, 6)
    for dim, parts in pieces:
        heights = jnp.exp(jax.random.uniform(jax.random.fold_in(own, dim), (parts,), jnp.float32, smallest / len(pieces), high / len(pieces)))
        level = level * jnp.repeat(heights, shape[dim] // parts).reshape([-1 if axis == dim else 1 for axis in range(len(shape))])
    return level


def setup_inputs(seed: int = 0) -> dict:
    key_list = jax.random.split(jax.random.key(seed), 4)
    return {
        "arrival": jnp.clip(4.0 * jax.random.uniform(key_list[0], (SCEN, PINS), jnp.float32) ** levels(key_list[0], (SCEN, PINS), ((1, 8),), -0.2, 0.2), 0.0, 4.0),
        "delay": draw_delay(jax.random.fold_in(key_list[3], 71), 0),
        "occupancy": draw_occupancy(jax.random.fold_in(key_list[3], 71), 0),
    }


def level_max(times, delay_level, flags):
    width = min(32, TILE)
    turns = PINS // width

    def step(best, index):
        start = (index * width).astype(jnp.int32)
        part_a = lax.dynamic_slice_in_dim(times, start, width, 1)
        part_d = lax.dynamic_slice_in_dim(delay_level, start, width, 0).astype(jnp.float32)
        tile_row = lax.dynamic_index_in_dim(flags, (start // TILE).astype(jnp.int32), 0, keepdims=False)
        keep = jnp.repeat(tile_row > 0, TILE)
        masked = jnp.where(keep[None, :], part_d, jnp.float32(-1e9))
        return jnp.maximum(best, jnp.max(part_a[:, :, None] + masked[None, :, :], axis=1)), None

    init = jnp.full((times.shape[0], PINS), -1e9, jnp.float32)
    best, unused = lax.scan(step, init, jnp.arange(turns, dtype=jnp.int32))
    return best


def reference(arrival, delay, occupancy):
    times = arrival
    for level in range(LEVELS):
        times = level_max(times, delay[level], occupancy[level])
    return times, jnp.max(times, axis=1)
```

```python
import functools

import jax
import jax.numpy as jnp
from jax import lax
from jax.experimental import pallas as pl
from jax.experimental.pallas import tpu as pltpu
from jax.sharding import PartitionSpec as P

MESH = pl.DeviceIdType.MESH
LANES = 128
LOW = -1000000000.0


def kernel(
    rows, cols, arrival_ref, delay_hbm, occ_ref, out_ref, worst_ref,
    delay_ref, wide_ref, part_ref, pair_ref, comb_ref, rs_ref, fin_ref, times_ref, peak_ref,
    load_sem, pair_send, pair_recv, rs_send, rs_recv, times_send, times_recv, peak_send, peak_recv,
):
    level_count, tile, width = delay_hbm.shape
    scenarios = arrival_ref.shape[0]
    ratio = cols // rows
    groups, ss, sp = rows, fin_ref.shape[1], fin_ref.shape[2]
    pin_groups = tile // sp
    scen_groups = scenarios // ss
    chunks = tile // LANES
    sub = sp // LANES
    row = lax.axis_index("row")
    col = lax.axis_index("col")
    z = col // ratio
    p = col % ratio

    def load(level):
        return pltpu.make_async_copy(delay_hbm.at[level], delay_ref.at[level], load_sem.at[level])

    for level in range(level_count):
        load(level).start()

    def widen(level):
        def step(i, carry):
            at = pl.ds(pl.multiple_of(i * 64, 64), 64)
            wide_ref[level, at, :] = delay_ref[level, at, :].astype(jnp.float32)
            return carry

        lax.fori_loop(0, tile // 64, step, 0)

    for g in range(scen_groups):
        for k in range(pin_groups):
            times_ref[0, g * pin_groups + k] = arrival_ref[g * ss:(g + 1) * ss, k * sp:(k + 1) * sp]
    load(0).wait()
    widen(0)

    def compute(level, q):
        lanes = pl.ds(pl.multiple_of(q * tile, LANES), tile)

        def step(chunk, best):
            k = chunk // sub
            at = pl.ds(pl.multiple_of((chunk % sub) * LANES, LANES), LANES)
            part_t = jnp.concatenate([times_ref[level, g * pin_groups + k, :, at] for g in range(scen_groups)], axis=0)
            for i in range(LANES):
                line = wide_ref[level, pl.ds(chunk * LANES + i, 1), lanes]
                best = jnp.maximum(best, part_t[:, i:i + 1] + line)
            return best

        best = lax.fori_loop(0, chunks, step, jnp.full((scenarios, tile), LOW, jnp.float32))
        flag = occ_ref[level, col, row * ratio + q]
        best = jnp.where(flag > 0, best, jnp.float32(LOW))
        for g in range(scen_groups):
            for k in range(pin_groups):
                part_ref[level, q, g * pin_groups + k] = best[g * ss:(g + 1) * ss, k * sp:(k + 1) * sp]

    def pair_copy(level, q):
        return pltpu.make_async_remote_copy(
            src_ref=part_ref.at[level, q], dst_ref=pair_ref.at[level, p],
            send_sem=pair_send.at[level, q], recv_sem=pair_recv.at[level, p],
            device_id=(row, z * ratio + q), device_id_type=MESH)

    def pair_arrival(level, q):
        return pltpu.make_async_remote_copy(
            src_ref=part_ref.at[level, q], dst_ref=pair_ref.at[level, q],
            send_sem=pair_send.at[level, q], recv_sem=pair_recv.at[level, q],
            device_id=(row, z * ratio + q), device_id_type=MESH)

    def rs_copy(level, other):
        return pltpu.make_async_remote_copy(
            src_ref=comb_ref.at[level, other], dst_ref=rs_ref.at[level, z],
            send_sem=rs_send.at[level, other], recv_sem=rs_recv.at[level, z],
            device_id=(row, other * ratio + p), device_id_type=MESH)

    def rs_arrival(level, other):
        return pltpu.make_async_remote_copy(
            src_ref=comb_ref.at[level, other], dst_ref=rs_ref.at[level, other],
            send_sem=rs_send.at[level, other], recv_sem=rs_recv.at[level, other],
            device_id=(row, other * ratio + p), device_id_type=MESH)

    def times_copy(level, to):
        return pltpu.make_async_remote_copy(
            src_ref=fin_ref.at[level], dst_ref=times_ref.at[level + 1, z],
            send_sem=times_send.at[level, to], recv_sem=times_recv.at[level, z],
            device_id=(to, row * ratio + p), device_id_type=MESH)

    def times_arrival(level, source):
        return pltpu.make_async_remote_copy(
            src_ref=fin_ref.at[level], dst_ref=times_ref.at[level + 1, source],
            send_sem=times_send.at[level, 0], recv_sem=times_recv.at[level, source],
            device_id=(z, source * ratio + p), device_id_type=MESH)

    def one_level(level, carry):
        for n in range(1, ratio):
            q = lax.rem(p + n, ratio)
            compute(level, q)
            pair_copy(level, q).start()
        compute(level, p)
        for n in range(1, ratio):
            pair_arrival(level, lax.rem(p + n, ratio)).wait_recv()

        total = part_ref[level, p]
        for n in range(1, ratio):
            total = jnp.maximum(total, pair_ref[level, lax.rem(p + n, ratio)])
        comb_ref[level] = total
        for n in range(1, groups):
            rs_copy(level, lax.rem(z + n, groups)).start()

        @pl.when(level + 1 < level_count)
        def _():
            load(level + 1).wait()
            widen(level + 1)

        total = comb_ref[level, z]
        for n in range(1, groups):
            other = lax.rem(z + n, groups)
            rs_arrival(level, other).wait_recv()
            total = jnp.maximum(total, rs_ref[level, other])
        fin_ref[level] = total
        for n in range(1, rows):
            times_copy(level, lax.rem(row + n, rows)).start()

        @pl.when(row != z)
        def _():
            times_copy(level, row).start()

        @pl.when(row == z)
        def _():
            times_ref[level + 1, z] = fin_ref[level]

        for n in range(1, ratio):
            pair_copy(level, lax.rem(p + n, ratio)).wait_send()
        for n in range(1, groups):
            rs_copy(level, lax.rem(z + n, groups)).wait_send()
        for n in range(1, groups):
            times_arrival(level, lax.rem(z + n, groups)).wait_recv()

        @pl.when(row != z)
        def _():
            times_arrival(level, z).wait_recv()
            times_copy(level, row).wait_send()

        for n in range(1, rows):
            times_copy(level, lax.rem(row + n, rows)).wait_send()
        return carry

    lax.fori_loop(0, level_count, one_level, 0)

    lane = lax.broadcasted_iota(jnp.int32, (ss, LANES), 1)
    line = lax.broadcasted_iota(jnp.int32, (ss, LANES), 0)
    peak = jnp.full((1, LANES), LOW, jnp.float32)
    for g in range(scen_groups):
        for k in range(pin_groups):
            value = times_ref[level_count, g * pin_groups + k]
            out_ref[g * ss:(g + 1) * ss, k * sp:(k + 1) * sp] = value
            top = jnp.max(value, axis=1, keepdims=True)
            spread = jnp.where(lane == line + g * ss, top, jnp.float32(LOW))
            peak = jnp.maximum(peak, jnp.max(spread, axis=0, keepdims=True))

    peak_ref[col] = peak

    def peak_copy(other):
        return pltpu.make_async_remote_copy(
            src_ref=peak_ref.at[col], dst_ref=peak_ref.at[col],
            send_sem=peak_send.at[other], recv_sem=peak_recv.at[col],
            device_id=(row, other), device_id_type=MESH)

    def peak_arrival(other):
        return pltpu.make_async_remote_copy(
            src_ref=peak_ref.at[col], dst_ref=peak_ref.at[other],
            send_sem=peak_send.at[other], recv_sem=peak_recv.at[other],
            device_id=(row, other), device_id_type=MESH)

    for n in range(1, cols):
        peak_copy(lax.rem(col + n, cols)).start()
    for n in range(1, cols):
        other = lax.rem(col + n, cols)
        peak_arrival(other).wait_recv()
        peak = jnp.maximum(peak, peak_ref[other])
    worst_ref[...] = peak
    for n in range(1, cols):
        peak_copy(lax.rem(col + n, cols)).wait_send()


def shards(arrival, delay, occupancy):
    rows, cols = lax.axis_size("row"), lax.axis_size("col")
    scenarios, tile = arrival.shape
    level_count, _, width = delay.shape
    ratio = cols // rows
    scen_groups = min(rows, scenarios // 16)
    pin_groups = rows // scen_groups
    ss, sp = scenarios // scen_groups, tile // pin_groups
    vmem = pl.BlockSpec(memory_space=pltpu.VMEM)
    f32 = jnp.float32
    dma = pltpu.SemaphoreType.DMA
    times, worst = pl.pallas_call(
        functools.partial(kernel, rows, cols),
        out_shape=(
            jax.ShapeDtypeStruct((scenarios, tile), f32),
            jax.ShapeDtypeStruct((1, LANES), f32),
        ),
        in_specs=[vmem, pl.BlockSpec(memory_space=pl.ANY), pl.BlockSpec(memory_space=pltpu.SMEM)],
        out_specs=(vmem, vmem),
        scratch_shapes=[
            pltpu.VMEM((level_count, tile, width), delay.dtype),
            pltpu.VMEM((level_count, tile, width), f32),
            pltpu.VMEM((level_count, ratio, rows, ss, sp), f32),
            pltpu.VMEM((level_count, ratio, rows, ss, sp), f32),
            pltpu.VMEM((level_count, rows, ss, sp), f32),
            pltpu.VMEM((level_count, rows, ss, sp), f32),
            pltpu.VMEM((level_count, ss, sp), f32),
            pltpu.VMEM((level_count + 1, rows, ss, sp), f32),
            pltpu.VMEM((cols, 1, LANES), f32),
            dma((level_count,)),
            dma((level_count, ratio)), dma((level_count, ratio)),
            dma((level_count, rows)), dma((level_count, rows)),
            dma((level_count, rows)), dma((level_count, rows)),
            dma((cols,)), dma((cols,)),
        ],
        compiler_params=pltpu.CompilerParams(has_side_effects=True, vmem_limit_bytes=48 * 1024 * 1024),
    )(arrival, delay, occupancy)
    return times, worst[0, :scenarios]


def solution(mesh):
    placed = (P(None, "col"), P(None, "col", "row"), P())
    return jax.shard_map(
        shards, mesh=mesh, in_specs=placed, out_specs=(P(None, "col"), P()), check_vma=False
    )
```

```python
import functools

import jax
import jax.numpy as jnp
from jax import lax
from jax.experimental import pallas as pl
from jax.experimental.pallas import tpu as pltpu
from jax.sharding import PartitionSpec as P

MESH = pl.DeviceIdType.MESH
LANES = 128
GROUP = 32
HALVES = 2
LOW = -1000000000.0


def kernel(
    rows, cols, arrival_ref, delay_hbm, occ_ref, out_ref, worst_ref,
    delay_ref, wide_ref, spread_ref, acc_ref, part_ref, pair_ref, comb_ref, rs_ref, fin_ref, times_ref, peak_ref,
    load_sem, pair_send, pair_recv, rs_send, rs_recv, times_send, times_recv, peak_send, peak_recv,
):
    level_count, tile, width = delay_hbm.shape
    scenarios = arrival_ref.shape[0]
    ratio = cols // rows
    slices, ss, sp = rows, fin_ref.shape[2], fin_ref.shape[3]
    half = tile // HALVES
    pin_groups = half // sp
    scen_groups = scenarios // ss
    group_count = half // GROUP
    per_chunk = LANES // GROUP
    row = lax.axis_index("row")
    col = lax.axis_index("col")
    z = col // ratio
    p = col % ratio

    def load(level):
        return pltpu.make_async_copy(delay_hbm.at[level], delay_ref.at[level], load_sem.at[level])

    for level in range(level_count):
        load(level).start()

    def widen(level):
        def step(i, carry):
            at = pl.ds(pl.multiple_of(i * 64, 64), 64)
            wide_ref[level, pl.ds(i * 8, 8)] = delay_ref[level, at, :].astype(jnp.float32).reshape(8, 8, width)
            return carry

        lax.fori_loop(0, tile // 64, step, 0)

    for h in range(HALVES):
        for g in range(scen_groups):
            for k in range(pin_groups):
                start = h * half + k * sp
                times_ref[0, h, g * pin_groups + k] = arrival_ref[g * ss:(g + 1) * ss, start:start + sp]
    load(0).wait()
    widen(0)

    def group_times(level, h, n):
        chunk = n // per_chunk
        k = chunk // (sp // LANES)
        at = pl.ds(pl.multiple_of((chunk % (sp // LANES)) * LANES, LANES), LANES)
        value = jnp.concatenate([times_ref[level, h, g * pin_groups + k, :, at] for g in range(scen_groups)], axis=0)
        return pltpu.roll(value, LANES - (n % per_chunk) * GROUP, 1)

    def spread(value, n, i):
        spread_ref[n * GROUP + i] = jnp.broadcast_to(value[:, i:i + 1], (scenarios, LANES))

    def fold(level, n, i, lanes, best):
        line = wide_ref[level, n * (GROUP // 8) + i // 8, i % 8:i % 8 + 1, lanes]
        return jnp.maximum(best, jnp.concatenate([spread_ref[n * GROUP + i]] * (half // LANES), axis=1) + line)

    def lanes_of(q, h):
        return pl.ds(pl.multiple_of(q * tile + h * half, LANES), half)

    def fused(level, q, h):
        value = group_times(level, h, 0)
        base = h * group_count
        for i in range(GROUP):
            spread(value, base, i)

        def step(n, carry):
            later = jnp.minimum(n + 1, group_count - 1)
            value = group_times(level, h, later)
            for j in range(HALVES):
                lanes = lanes_of(q, j)
                best = acc_ref[j]
                for i in range(GROUP):
                    best = fold(level, base + n, i, lanes, best)
                    if i % HALVES == 0:
                        spread(value, base + later, j * (GROUP // HALVES) + i // HALVES)
                acc_ref[j] = best
            return carry

        lax.fori_loop(0, group_count, step, 0)

    def put(level, q, h, best):
        flag = occ_ref[level, col, row * ratio + q]
        best = jnp.where(flag > 0, best, jnp.float32(LOW))
        for g in range(scen_groups):
            for k in range(pin_groups):
                part_ref[level, q, h, g * pin_groups + k] = best[g * ss:(g + 1) * ss, k * sp:(k + 1) * sp]

    def dense(level, q, h):
        lanes = lanes_of(q, h)

        def step(n, best):
            for i in range(GROUP):
                best = fold(level, n, i, lanes, best)
            return best

        best = lax.fori_loop(0, tile // GROUP, step, jnp.full((scenarios, half), LOW, jnp.float32))
        put(level, q, h, best)

    def pair_copy(level, h, q, slot):
        return pltpu.make_async_remote_copy(
            src_ref=part_ref.at[level, q, h], dst_ref=pair_ref.at[level, slot, h],
            send_sem=pair_send.at[level, h, q], recv_sem=pair_recv.at[level, h, slot],
            device_id=(row, z * ratio + q), device_id_type=MESH)

    def rs_copy(level, h, other, slot):
        return pltpu.make_async_remote_copy(
            src_ref=comb_ref.at[level, h, other], dst_ref=rs_ref.at[level, h, slot],
            send_sem=rs_send.at[level, h, other], recv_sem=rs_recv.at[level, h, slot],
            device_id=(row, other * ratio + p), device_id_type=MESH)

    def times_copy(level, h, to, slot):
        return pltpu.make_async_remote_copy(
            src_ref=fin_ref.at[level, h], dst_ref=times_ref.at[level + 1, h, slot],
            send_sem=times_send.at[level, h, to], recv_sem=times_recv.at[level, h, slot],
            device_id=(to, row * ratio + p), device_id_type=MESH)

    def wait_times(level, h):
        for n in range(1, slices):
            times_copy(level, h, 0, lax.rem(z + n, slices)).wait_recv()

        @pl.when(row != z)
        def _():
            times_copy(level, h, 0, z).wait_recv()

    def one_level(level, carry):
        order = [lax.rem(p + n, ratio) for n in range(1, ratio)] + [p]
        for h in range(HALVES):
            acc_ref[h] = jnp.full((scenarios, half), LOW, jnp.float32)
        for h in range(HALVES):
            @pl.when(level > 0)
            def _():
                wait_times(level - 1, h)

            fused(level, order[0], h)

        for n, q in enumerate(order[:-1]):
            for h in range(HALVES):
                if n == 0:
                    put(level, q, h, acc_ref[h])
                else:
                    dense(level, q, h)
                pair_copy(level, h, q, p).start()

        for h in range(HALVES):
            if ratio == 1:
                put(level, p, h, acc_ref[h])
            else:
                dense(level, p, h)
            total = part_ref[level, p, h]
            for q in order[:-1]:
                pair_copy(level, h, q, q).wait_recv()
                total = jnp.maximum(total, pair_ref[level, q, h])
            comb_ref[level, h] = total
            for n in range(1, slices):
                rs_copy(level, h, lax.rem(z + n, slices), z).start()

        @pl.when(level + 1 < level_count)
        def _():
            load(level + 1).wait()
            widen(level + 1)

        for h in range(HALVES):
            total = comb_ref[level, h, z]
            for n in range(1, slices):
                other = lax.rem(z + n, slices)
                rs_copy(level, h, other, other).wait_recv()
                total = jnp.maximum(total, rs_ref[level, h, other])
            fin_ref[level, h] = total
            for n in range(1, rows):
                times_copy(level, h, lax.rem(row + n, rows), z).start()

            @pl.when(row != z)
            def _():
                times_copy(level, h, row, z).start()

            @pl.when(row == z)
            def _():
                times_ref[level + 1, h, z] = fin_ref[level, h]

        return carry

    lax.fori_loop(0, level_count, one_level, 0)

    lane = lax.broadcasted_iota(jnp.int32, (ss, LANES), 1)
    line = lax.broadcasted_iota(jnp.int32, (ss, LANES), 0)
    peak = jnp.full((1, LANES), LOW, jnp.float32)
    for h in range(HALVES):
        wait_times(level_count - 1, h)
        for g in range(scen_groups):
            for k in range(pin_groups):
                value = times_ref[level_count, h, g * pin_groups + k]
                start = h * half + k * sp
                out_ref[g * ss:(g + 1) * ss, start:start + sp] = value
                top = jnp.max(value, axis=1, keepdims=True)
                shown = jnp.where(lane == line + g * ss, top, jnp.float32(LOW))
                peak = jnp.maximum(peak, jnp.max(shown, axis=0, keepdims=True))

    peak_ref[col] = peak

    def peak_copy(other, slot):
        return pltpu.make_async_remote_copy(
            src_ref=peak_ref.at[col], dst_ref=peak_ref.at[slot],
            send_sem=peak_send.at[other], recv_sem=peak_recv.at[slot],
            device_id=(row, other), device_id_type=MESH)

    for n in range(1, cols):
        peak_copy(lax.rem(col + n, cols), col).start()

    def settle(level, carry):
        for h in range(HALVES):
            for n in range(1, ratio):
                pair_copy(level, h, lax.rem(p + n, ratio), p).wait_send()
            for n in range(1, slices):
                rs_copy(level, h, lax.rem(z + n, slices), z).wait_send()
            for n in range(1, rows):
                times_copy(level, h, lax.rem(row + n, rows), z).wait_send()

            @pl.when(row != z)
            def _():
                times_copy(level, h, row, z).wait_send()

        return carry

    lax.fori_loop(0, level_count, settle, 0)

    for n in range(1, cols):
        other = lax.rem(col + n, cols)
        peak_copy(other, other).wait_recv()
        peak = jnp.maximum(peak, peak_ref[other])
    worst_ref[...] = peak
    for n in range(1, cols):
        peak_copy(lax.rem(col + n, cols), col).wait_send()


def shards(arrival, delay, occupancy):
    rows, cols = lax.axis_size("row"), lax.axis_size("col")
    scenarios, tile = arrival.shape
    level_count, _, width = delay.shape
    ratio = cols // rows
    half = tile // HALVES
    scen_groups = min(rows, scenarios // 8)
    pin_groups = rows // scen_groups
    ss, sp = scenarios // scen_groups, half // pin_groups
    vmem = pl.BlockSpec(memory_space=pltpu.VMEM)
    f32 = jnp.float32
    dma = pltpu.SemaphoreType.DMA
    times, worst = pl.pallas_call(
        functools.partial(kernel, rows, cols),
        out_shape=(
            jax.ShapeDtypeStruct((scenarios, tile), f32),
            jax.ShapeDtypeStruct((1, LANES), f32),
        ),
        in_specs=[vmem, pl.BlockSpec(memory_space=pltpu.HBM), pl.BlockSpec(memory_space=pltpu.SMEM)],
        out_specs=(vmem, vmem),
        scratch_shapes=[
            pltpu.VMEM((level_count, tile, width), delay.dtype),
            pltpu.VMEM((level_count, tile // 8, 8, width), f32),
            pltpu.VMEM((tile, scenarios, LANES), f32),
            pltpu.VMEM((HALVES, scenarios, half), f32),
            pltpu.VMEM((level_count, ratio, HALVES, rows, ss, sp), f32),
            pltpu.VMEM((level_count, ratio, HALVES, rows, ss, sp), f32),
            pltpu.VMEM((level_count, HALVES, rows, ss, sp), f32),
            pltpu.VMEM((level_count, HALVES, rows, ss, sp), f32),
            pltpu.VMEM((level_count, HALVES, ss, sp), f32),
            pltpu.VMEM((level_count + 1, HALVES, rows, ss, sp), f32),
            pltpu.VMEM((cols, 1, LANES), f32),
            dma((level_count,)),
            dma((level_count, HALVES, ratio)), dma((level_count, HALVES, ratio)),
            dma((level_count, HALVES, rows)), dma((level_count, HALVES, rows)),
            dma((level_count, HALVES, rows)), dma((level_count, HALVES, rows)),
            dma((cols,)), dma((cols,)),
        ],
        compiler_params=pltpu.CompilerParams(has_side_effects=True, vmem_limit_bytes=60 * 1024 * 1024),
    )(arrival, delay, occupancy)
    return times, worst[0, :scenarios]


def solution(mesh):
    placed = (P(None, "col"), P(None, "col", "row"), P())
    return jax.shard_map(
        shards, mesh=mesh, in_specs=placed, out_specs=(P(None, "col"), P()), check_vma=False
    )
```

```python
import functools

import jax
import jax.numpy as jnp
from jax import lax
from jax.experimental import pallas as pl
from jax.experimental.pallas import tpu as pltpu
from jax.sharding import PartitionSpec as P

MESH = pl.DeviceIdType.MESH
LANES = 128
GROUP = 32
LAG = 3
LOW = -1000000000.0


def kernel(
    rows, cols, arrival_ref, delay_hbm, occ_ref, out_ref, worst_ref,
    delay_ref, wide_ref, part_ref, pair_ref, comb_ref, rs_ref, fin_ref, times_ref, peak_ref,
    load_sem, pair_send, pair_recv, rs_send, rs_recv, times_send, times_recv, peak_send, peak_recv,
):
    level_count, tile, width = delay_hbm.shape
    ratio = cols // rows
    groups, slices, ss, sp = times_ref.shape[1:]
    pin_groups = tile // sp
    sub = slices // pin_groups
    gscen = sub * ss
    row = lax.axis_index("row")
    col = lax.axis_index("col")
    z = col // ratio
    p = col % ratio

    def load(level):
        return pltpu.make_async_copy(delay_hbm.at[level], delay_ref.at[level], load_sem.at[level])

    for level in range(level_count):
        load(level).start()

    def widen(level):
        def step(i, carry):
            at = pl.ds(pl.multiple_of(i * 64, 64), 64)
            wide_ref[level, pl.ds(i * 8, 8)] = delay_ref[level, at, :].astype(jnp.float32).reshape(8, 8, width)
            return carry

        lax.fori_loop(0, tile // 64, step, 0)

    for h in range(groups):
        for g in range(sub):
            for k in range(pin_groups):
                start = h * gscen + g * ss
                times_ref[0, h, g * pin_groups + k] = arrival_ref[start:start + ss, k * sp:(k + 1) * sp]
    load(0).wait()
    widen(0)

    def compute(level, h):
        def step(n, best):
            k = n // (sp // GROUP)
            value = jnp.concatenate([times_ref[level, h, g * pin_groups + k] for g in range(sub)], axis=0)
            if GROUP < sp:
                value = pltpu.roll(value, sp - (n % (sp // GROUP)) * GROUP, 1)
            for i in range(GROUP):
                line = wide_ref[level, n * (GROUP // 8) + i // 8, i % 8:i % 8 + 1, :]
                spread = jnp.broadcast_to(value[:, i:i + 1], (gscen, LANES))
                best = jnp.maximum(best, jnp.concatenate([spread] * (width // LANES), axis=1) + line)
            return best

        best = lax.fori_loop(0, tile // GROUP, step, jnp.full((gscen, width), LOW, jnp.float32))
        for q in range(ratio):
            flag = occ_ref[level, col, row * ratio + q]
            for g in range(sub):
                for k in range(pin_groups):
                    start = q * tile + k * sp
                    piece = best[g * ss:(g + 1) * ss, start:start + sp]
                    part_ref[level, q, h, g * pin_groups + k] = jnp.where(flag > 0, piece, jnp.float32(LOW))

    def pair_copy(level, h, q, slot):
        return pltpu.make_async_remote_copy(
            src_ref=part_ref.at[level, q, h], dst_ref=pair_ref.at[level, slot, h],
            send_sem=pair_send.at[level, h, q], recv_sem=pair_recv.at[level, h, slot],
            device_id=(row, z * ratio + q), device_id_type=MESH)

    def rs_copy(level, h, other, slot):
        return pltpu.make_async_remote_copy(
            src_ref=comb_ref.at[level, h, other], dst_ref=rs_ref.at[level, h, slot],
            send_sem=rs_send.at[level, h, other], recv_sem=rs_recv.at[level, h, slot],
            device_id=(row, other * ratio + p), device_id_type=MESH)

    def times_copy(level, h, to, slot):
        return pltpu.make_async_remote_copy(
            src_ref=fin_ref.at[level, h], dst_ref=times_ref.at[level + 1, h, slot],
            send_sem=times_send.at[level, h, to], recv_sem=times_recv.at[level, h, slot],
            device_id=(to, row * ratio + p), device_id_type=MESH)

    def wait_times(level, h):
        for n in range(1, slices):
            times_copy(level, h, 0, lax.rem(z + n, slices)).wait_recv()

        @pl.when(row != z)
        def _():
            times_copy(level, h, 0, z).wait_recv()

    def combine(level, h):
        total = part_ref[level, p, h]
        for n in range(1, ratio):
            q = lax.rem(p + n, ratio)
            pair_copy(level, h, q, q).wait_recv()
            total = jnp.maximum(total, pair_ref[level, q, h])
        comb_ref[level, h] = total
        for n in range(1, slices):
            rs_copy(level, h, lax.rem(z + n, slices), z).start()

    def finish(level, h):
        total = comb_ref[level, h, z]
        for n in range(1, slices):
            other = lax.rem(z + n, slices)
            rs_copy(level, h, other, other).wait_recv()
            total = jnp.maximum(total, rs_ref[level, h, other])
        fin_ref[level, h] = total
        for n in range(1, rows):
            times_copy(level, h, lax.rem(row + n, rows), z).start()

        @pl.when(row != z)
        def _():
            times_copy(level, h, row, z).start()

        @pl.when(row == z)
        def _():
            times_ref[level + 1, h, z] = fin_ref[level, h]

    def one_level(level, carry):
        for h in range(groups):
            @pl.when(level > 0)
            def _():
                wait_times(level - 1, h)

            compute(level, h)
            for n in range(1, ratio):
                pair_copy(level, h, lax.rem(p + n, ratio), p).start()
            if h >= 1:
                combine(level, h - 1)
            if h >= LAG:
                finish(level, h - LAG)

        @pl.when(level + 1 < level_count)
        def _():
            load(level + 1).wait()
            widen(level + 1)

        combine(level, groups - 1)
        for h in range(max(0, groups - LAG), groups):
            finish(level, h)
        return carry

    lax.fori_loop(0, level_count, one_level, 0)

    lane = lax.broadcasted_iota(jnp.int32, (ss, LANES), 1)
    line = lax.broadcasted_iota(jnp.int32, (ss, LANES), 0)
    peak = jnp.full((1, LANES), LOW, jnp.float32)
    for h in range(groups):
        wait_times(level_count - 1, h)
        for g in range(sub):
            for k in range(pin_groups):
                value = times_ref[level_count, h, g * pin_groups + k]
                start = h * gscen + g * ss
                out_ref[start:start + ss, k * sp:(k + 1) * sp] = value
                top = jnp.max(value, axis=1, keepdims=True)
                shown = jnp.where(lane == line + start, top, jnp.float32(LOW))
                peak = jnp.maximum(peak, jnp.max(shown, axis=0, keepdims=True))

    peak_ref[col] = peak

    def peak_copy(other, slot):
        return pltpu.make_async_remote_copy(
            src_ref=peak_ref.at[col], dst_ref=peak_ref.at[slot],
            send_sem=peak_send.at[other], recv_sem=peak_recv.at[slot],
            device_id=(row, other), device_id_type=MESH)

    for n in range(1, cols):
        peak_copy(lax.rem(col + n, cols), col).start()

    def settle(level, carry):
        for h in range(groups):
            for n in range(1, ratio):
                pair_copy(level, h, lax.rem(p + n, ratio), p).wait_send()
            for n in range(1, slices):
                rs_copy(level, h, lax.rem(z + n, slices), z).wait_send()
            for n in range(1, rows):
                times_copy(level, h, lax.rem(row + n, rows), z).wait_send()

            @pl.when(row != z)
            def _():
                times_copy(level, h, row, z).wait_send()

        return carry

    lax.fori_loop(0, level_count, settle, 0)

    for n in range(1, cols):
        other = lax.rem(col + n, cols)
        peak_copy(other, other).wait_recv()
        peak = jnp.maximum(peak, peak_ref[other])
    worst_ref[...] = peak
    for n in range(1, cols):
        peak_copy(lax.rem(col + n, cols), col).wait_send()


def shards(arrival, delay, occupancy):
    rows, cols = lax.axis_size("row"), lax.axis_size("col")
    scenarios, tile = arrival.shape
    level_count, _, width = delay.shape
    ratio = cols // rows
    sp = LANES
    pin_groups = tile // sp
    sub = rows // pin_groups
    ss = max(8, 16 // sub)
    groups = scenarios // (sub * ss)
    vmem = pl.BlockSpec(memory_space=pltpu.VMEM)
    f32 = jnp.float32
    dma = pltpu.SemaphoreType.DMA
    times, worst = pl.pallas_call(
        functools.partial(kernel, rows, cols),
        out_shape=(
            jax.ShapeDtypeStruct((scenarios, tile), f32),
            jax.ShapeDtypeStruct((1, LANES), f32),
        ),
        in_specs=[vmem, pl.BlockSpec(memory_space=pltpu.HBM), pl.BlockSpec(memory_space=pltpu.SMEM)],
        out_specs=(vmem, vmem),
        scratch_shapes=[
            pltpu.VMEM((level_count, tile, width), delay.dtype),
            pltpu.VMEM((level_count, tile // 8, 8, width), f32),
            pltpu.VMEM((level_count, ratio, groups, rows, ss, sp), f32),
            pltpu.VMEM((level_count, ratio, groups, rows, ss, sp), f32),
            pltpu.VMEM((level_count, groups, rows, ss, sp), f32),
            pltpu.VMEM((level_count, groups, rows, ss, sp), f32),
            pltpu.VMEM((level_count, groups, ss, sp), f32),
            pltpu.VMEM((level_count + 1, groups, rows, ss, sp), f32),
            pltpu.VMEM((cols, 1, LANES), f32),
            dma((level_count,)),
            dma((level_count, groups, ratio)), dma((level_count, groups, ratio)),
            dma((level_count, groups, rows)), dma((level_count, groups, rows)),
            dma((level_count, groups, rows)), dma((level_count, groups, rows)),
            dma((cols,)), dma((cols,)),
        ],
        compiler_params=pltpu.CompilerParams(has_side_effects=True, vmem_limit_bytes=60 * 1024 * 1024),
    )(arrival, delay, occupancy)
    return times, worst[0, :scenarios]


def solution(mesh):
    placed = (P(None, "col"), P(None, "col", "row"), P())
    return jax.shard_map(
        shards, mesh=mesh, in_specs=placed, out_specs=(P(None, "col"), P()), check_vma=False
    )
```

```python
import functools

import jax
import jax.numpy as jnp
from jax import lax
from jax.experimental import pallas as pl
from jax.experimental.pallas import tpu as pltpu
from jax.sharding import PartitionSpec as P

MESH = pl.DeviceIdType.MESH
LANES = 128
GROUP = 128
LAG = 3
LOW = -1000000000.0


def kernel(
    rows, cols, arrival_ref, delay_hbm, occ_ref, out_ref, worst_ref,
    delay_ref, wide_ref, part_ref, pair_ref, comb_ref, rs_ref, fin_ref, times_ref, peak_ref,
    load_sem, pair_send, pair_recv, rs_send, rs_recv, times_send, times_recv, peak_send, peak_recv,
):
    level_count, tile, width = delay_hbm.shape
    ratio = cols // rows
    groups, slices, ss, sp = times_ref.shape[1:]
    pin_groups = tile // sp
    sub = slices // pin_groups
    gscen = sub * ss
    row = lax.axis_index("row")
    col = lax.axis_index("col")
    z = col // ratio
    p = col % ratio

    def load(level):
        return pltpu.make_async_copy(delay_hbm.at[level], delay_ref.at[level], load_sem.at[level])

    for level in range(level_count):
        load(level).start()

    def widen(level):
        def step(i, carry):
            at = pl.ds(pl.multiple_of(i * 64, 64), 64)
            wide_ref[level, pl.ds(i * 8, 8)] = delay_ref[level, at, :].astype(jnp.float32).reshape(8, 8, width)
            return carry

        lax.fori_loop(0, tile // 64, step, 0)

    for h in range(groups):
        for g in range(sub):
            for k in range(pin_groups):
                start = h * gscen + g * ss
                times_ref[0, h, g * pin_groups + k] = arrival_ref[start:start + ss, k * sp:(k + 1) * sp]
    load(0).wait()
    widen(0)

    def compute(level, h):
        def step(n, best):
            k = n // (sp // GROUP)
            value = jnp.concatenate([times_ref[level, h, g * pin_groups + k] for g in range(sub)], axis=0)
            if GROUP < sp:
                value = pltpu.roll(value, sp - (n % (sp // GROUP)) * GROUP, 1)
            for i in range(GROUP):
                spread = jnp.broadcast_to(value[:, i:i + 1], (gscen, LANES))
                best = tuple(jnp.maximum(b, spread + wide_ref[level, n * (GROUP // 8) + i // 8, i % 8:i % 8 + 1, c * LANES:(c + 1) * LANES]) for c, b in enumerate(best))
            return best

        best = lax.fori_loop(0, tile // GROUP, step, (jnp.full((gscen, LANES), LOW, jnp.float32),) * (width // LANES))
        best = jnp.concatenate(best, axis=1)
        for q in range(ratio):
            flag = occ_ref[level, col, row * ratio + q]
            for g in range(sub):
                for k in range(pin_groups):
                    start = q * tile + k * sp
                    piece = best[g * ss:(g + 1) * ss, start:start + sp]
                    part_ref[level, q, h, g * pin_groups + k] = jnp.where(flag > 0, piece, jnp.float32(LOW))

    def pair_copy(level, h, q, slot):
        return pltpu.make_async_remote_copy(
            src_ref=part_ref.at[level, q, h], dst_ref=pair_ref.at[level, slot, h],
            send_sem=pair_send.at[level, h, q], recv_sem=pair_recv.at[level, h, slot],
            device_id=(row, z * ratio + q), device_id_type=MESH)

    def rs_copy(level, h, other, slot):
        return pltpu.make_async_remote_copy(
            src_ref=comb_ref.at[level, h, other], dst_ref=rs_ref.at[level, h, slot],
            send_sem=rs_send.at[level, h, other], recv_sem=rs_recv.at[level, h, slot],
            device_id=(row, other * ratio + p), device_id_type=MESH)

    def times_copy(level, h, to, slot):
        return pltpu.make_async_remote_copy(
            src_ref=fin_ref.at[level, h], dst_ref=times_ref.at[level + 1, h, slot],
            send_sem=times_send.at[level, h, to], recv_sem=times_recv.at[level, h, slot],
            device_id=(to, row * ratio + p), device_id_type=MESH)

    def wait_times(level, h):
        for n in range(1, slices):
            times_copy(level, h, 0, lax.rem(z + n, slices)).wait_recv()

        @pl.when(row != z)
        def _():
            times_copy(level, h, 0, z).wait_recv()

    def combine(level, h):
        total = part_ref[level, p, h]
        for n in range(1, ratio):
            q = lax.rem(p + n, ratio)
            pair_copy(level, h, q, q).wait_recv()
            total = jnp.maximum(total, pair_ref[level, q, h])
        comb_ref[level, h] = total
        for n in range(1, slices):
            rs_copy(level, h, lax.rem(z + n, slices), z).start()

    def finish(level, h):
        total = comb_ref[level, h, z]
        for n in range(1, slices):
            other = lax.rem(z + n, slices)
            rs_copy(level, h, other, other).wait_recv()
            total = jnp.maximum(total, rs_ref[level, h, other])
        fin_ref[level, h] = total
        for n in range(1, rows):
            times_copy(level, h, lax.rem(row + n, rows), z).start()

        @pl.when(row != z)
        def _():
            times_copy(level, h, row, z).start()

        @pl.when(row == z)
        def _():
            times_ref[level + 1, h, z] = fin_ref[level, h]

    def one_level(level, carry):
        for h in range(groups):
            @pl.when(level > 0)
            def _():
                wait_times(level - 1, h)

            compute(level, h)
            for n in range(1, ratio):
                pair_copy(level, h, lax.rem(p + n, ratio), p).start()
            if h >= 1:
                combine(level, h - 1)
            if h >= LAG:
                finish(level, h - LAG)

        @pl.when(level + 1 < level_count)
        def _():
            load(level + 1).wait()
            widen(level + 1)

        combine(level, groups - 1)
        for h in range(max(0, groups - LAG), groups):
            finish(level, h)
        return carry

    lax.fori_loop(0, level_count, one_level, 0)

    lane = lax.broadcasted_iota(jnp.int32, (ss, LANES), 1)
    line = lax.broadcasted_iota(jnp.int32, (ss, LANES), 0)
    peak = jnp.full((1, LANES), LOW, jnp.float32)
    for h in range(groups):
        wait_times(level_count - 1, h)
        for g in range(sub):
            for k in range(pin_groups):
                value = times_ref[level_count, h, g * pin_groups + k]
                start = h * gscen + g * ss
                out_ref[start:start + ss, k * sp:(k + 1) * sp] = value
                top = jnp.max(value, axis=1, keepdims=True)
                shown = jnp.where(lane == line + start, top, jnp.float32(LOW))
                peak = jnp.maximum(peak, jnp.max(shown, axis=0, keepdims=True))

    peak_ref[col] = peak

    def peak_copy(other, slot):
        return pltpu.make_async_remote_copy(
            src_ref=peak_ref.at[col], dst_ref=peak_ref.at[slot],
            send_sem=peak_send.at[other], recv_sem=peak_recv.at[slot],
            device_id=(row, other), device_id_type=MESH)

    for n in range(1, cols):
        peak_copy(lax.rem(col + n, cols), col).start()

    def settle(level, carry):
        for h in range(groups):
            for n in range(1, ratio):
                pair_copy(level, h, lax.rem(p + n, ratio), p).wait_send()
            for n in range(1, slices):
                rs_copy(level, h, lax.rem(z + n, slices), z).wait_send()
            for n in range(1, rows):
                times_copy(level, h, lax.rem(row + n, rows), z).wait_send()

            @pl.when(row != z)
            def _():
                times_copy(level, h, row, z).wait_send()

        return carry

    lax.fori_loop(0, level_count, settle, 0)

    for n in range(1, cols):
        other = lax.rem(col + n, cols)
        peak_copy(other, other).wait_recv()
        peak = jnp.maximum(peak, peak_ref[other])
    worst_ref[...] = peak
    for n in range(1, cols):
        peak_copy(lax.rem(col + n, cols), col).wait_send()


def shards(arrival, delay, occupancy):
    rows, cols = lax.axis_size("row"), lax.axis_size("col")
    scenarios, tile = arrival.shape
    level_count, _, width = delay.shape
    ratio = cols // rows
    sp = LANES
    pin_groups = tile // sp
    sub = rows // pin_groups
    ss = max(8, 16 // sub)
    groups = scenarios // (sub * ss)
    vmem = pl.BlockSpec(memory_space=pltpu.VMEM)
    f32 = jnp.float32
    dma = pltpu.SemaphoreType.DMA
    times, worst = pl.pallas_call(
        functools.partial(kernel, rows, cols),
        out_shape=(
            jax.ShapeDtypeStruct((scenarios, tile), f32),
            jax.ShapeDtypeStruct((1, LANES), f32),
        ),
        in_specs=[vmem, pl.BlockSpec(memory_space=pltpu.HBM), pl.BlockSpec(memory_space=pltpu.SMEM)],
        out_specs=(vmem, vmem),
        scratch_shapes=[
            pltpu.VMEM((level_count, tile, width), delay.dtype),
            pltpu.VMEM((level_count, tile // 8, 8, width), f32),
            pltpu.VMEM((level_count, ratio, groups, rows, ss, sp), f32),
            pltpu.VMEM((level_count, ratio, groups, rows, ss, sp), f32),
            pltpu.VMEM((level_count, groups, rows, ss, sp), f32),
            pltpu.VMEM((level_count, groups, rows, ss, sp), f32),
            pltpu.VMEM((level_count, groups, ss, sp), f32),
            pltpu.VMEM((level_count + 1, groups, rows, ss, sp), f32),
            pltpu.VMEM((cols, 1, LANES), f32),
            dma((level_count,)),
            dma((level_count, groups, ratio)), dma((level_count, groups, ratio)),
            dma((level_count, groups, rows)), dma((level_count, groups, rows)),
            dma((level_count, groups, rows)), dma((level_count, groups, rows)),
            dma((cols,)), dma((cols,)),
        ],
        compiler_params=pltpu.CompilerParams(has_side_effects=True, vmem_limit_bytes=60 * 1024 * 1024),
    )(arrival, delay, occupancy)
    return times, worst[0, :scenarios]


def solution(mesh):
    placed = (P(None, "col"), P(None, "col", "row"), P())
    return jax.shard_map(
        shards, mesh=mesh, in_specs=placed, out_specs=(P(None, "col"), P()), check_vma=False
    )
```

```python
import functools

import jax
import jax.numpy as jnp
from jax import lax
from jax.experimental import pallas as pl
from jax.experimental.pallas import tpu as pltpu
from jax.sharding import PartitionSpec as P

MESH = pl.DeviceIdType.MESH
LANES = 128
GROUP = 128
LAG = 3
LOW = -1000000000.0


def kernel(
    rows, cols, arrival_ref, delay_hbm, occ_ref, out_ref, worst_ref,
    delay_ref, wide_ref, part_ref, pair_ref, comb_ref, rs_ref, fin_ref, times_ref, peak_ref,
    load_sem, pair_send, pair_recv, rs_send, rs_recv, times_send, times_recv, peak_send, peak_recv,
):
    level_count, tile, width = delay_hbm.shape
    ratio = cols // rows
    groups, slices, ss, sp = times_ref.shape[1:]
    pin_groups = tile // sp
    sub = slices // pin_groups
    gscen = sub * ss
    row = lax.axis_index("row")
    col = lax.axis_index("col")
    z = col // ratio
    p = col % ratio

    barrier = pltpu.get_barrier_semaphore()

    def greet(to_row, to_col):
        pl.semaphore_signal(barrier, inc=1, device_id=(to_row, to_col), device_id_type=MESH)

    for n in range(1, cols):
        greet(row, lax.rem(col + n, cols))
    for n in range(1, rows):
        greet(lax.rem(row + n, rows), row * ratio + p)
        greet(z, lax.rem(z + n, slices) * ratio + p)

    @pl.when(row != z)
    def _():
        greet(row, row * ratio + p)
        greet(z, z * ratio + p)

    peers = cols - 1 + 2 * (rows - 1) + 2 * (row != z).astype(jnp.int32)

    def load(level):
        return pltpu.make_async_copy(delay_hbm.at[level], delay_ref.at[level], load_sem.at[level])

    for level in range(level_count):
        load(level).start()

    def widen(level):
        def step(i, carry):
            at = pl.ds(pl.multiple_of(i * 64, 64), 64)
            wide_ref[level, pl.ds(i * 8, 8)] = delay_ref[level, at, :].astype(jnp.float32).reshape(8, 8, width)
            return carry

        lax.fori_loop(0, tile // 64, step, 0)

    for h in range(groups):
        for g in range(sub):
            for k in range(pin_groups):
                start = h * gscen + g * ss
                times_ref[0, h, g * pin_groups + k] = arrival_ref[start:start + ss, k * sp:(k + 1) * sp]
    load(0).wait()
    widen(0)

    def compute(level, h, middle):
        def step(n, best):
            @pl.when(n == tile // GROUP // 2)
            def _():
                middle()

            k = n // (sp // GROUP)
            value = jnp.concatenate([times_ref[level, h, g * pin_groups + k] for g in range(sub)], axis=0)
            if GROUP < sp:
                value = pltpu.roll(value, sp - (n % (sp // GROUP)) * GROUP, 1)
            for i in range(GROUP):
                spread = jnp.broadcast_to(value[:, i:i + 1], (gscen, LANES))
                best = tuple(jnp.maximum(b, spread + wide_ref[level, n * (GROUP // 8) + i // 8, i % 8:i % 8 + 1, c * LANES:(c + 1) * LANES]) for c, b in enumerate(best))
            return best

        best = lax.fori_loop(0, tile // GROUP, step, (jnp.full((gscen, LANES), LOW, jnp.float32),) * (width // LANES))
        best = jnp.concatenate(best, axis=1)
        for q in range(ratio):
            flag = occ_ref[level, col, row * ratio + q]
            for g in range(sub):
                for k in range(pin_groups):
                    start = q * tile + k * sp
                    piece = best[g * ss:(g + 1) * ss, start:start + sp]
                    part_ref[level, q, h, g * pin_groups + k] = jnp.where(flag > 0, piece, jnp.float32(LOW))

    def pair_copy(level, h, q, slot):
        return pltpu.make_async_remote_copy(
            src_ref=part_ref.at[level, q, h], dst_ref=pair_ref.at[level, slot, h],
            send_sem=pair_send.at[level, h, q], recv_sem=pair_recv.at[level, h, slot],
            device_id=(row, z * ratio + q), device_id_type=MESH)

    def rs_copy(level, h, other, slot):
        return pltpu.make_async_remote_copy(
            src_ref=comb_ref.at[level, h, other], dst_ref=rs_ref.at[level, h, slot],
            send_sem=rs_send.at[level, h, other], recv_sem=rs_recv.at[level, h, slot],
            device_id=(row, other * ratio + p), device_id_type=MESH)

    def times_copy(level, h, to, slot):
        return pltpu.make_async_remote_copy(
            src_ref=fin_ref.at[level, h], dst_ref=times_ref.at[level + 1, h, slot],
            send_sem=times_send.at[level, h, to], recv_sem=times_recv.at[level, h, slot],
            device_id=(to, row * ratio + p), device_id_type=MESH)

    def wait_times(level, h):
        for n in range(1, slices):
            times_copy(level, h, 0, lax.rem(z + n, slices)).wait_recv()

        @pl.when(row != z)
        def _():
            times_copy(level, h, 0, z).wait_recv()

    def combine(level, h):
        total = part_ref[level, p, h]
        for n in range(1, ratio):
            q = lax.rem(p + n, ratio)
            pair_copy(level, h, q, q).wait_recv()
            total = jnp.maximum(total, pair_ref[level, q, h])
        comb_ref[level, h] = total
        for n in range(1, slices):
            rs_copy(level, h, lax.rem(z + n, slices), z).start()

    def finish(level, h):
        total = comb_ref[level, h, z]
        for n in range(1, slices):
            other = lax.rem(z + n, slices)
            rs_copy(level, h, other, other).wait_recv()
            total = jnp.maximum(total, rs_ref[level, h, other])
        fin_ref[level, h] = total
        for n in range(1, rows):
            times_copy(level, h, lax.rem(row + n, rows), z).start()

        @pl.when(row != z)
        def _():
            times_copy(level, h, row, z).start()

        @pl.when(row == z)
        def _():
            times_ref[level + 1, h, z] = fin_ref[level, h]

    def one_level(level, carry):
        for h in range(groups):
            @pl.when(level > 0)
            def _():
                wait_times(level - 1, h)

            def middle():
                if h >= 1:
                    combine(level, h - 1)
                else:
                    @pl.when(level > 0)
                    def _():
                        finish(level - 1, groups - 1)
                if h >= LAG:
                    finish(level, h - LAG)

            compute(level, h, middle)
            for n in range(1, ratio):
                pair_copy(level, h, lax.rem(p + n, ratio), p).start()

        @pl.when(level + 1 < level_count)
        def _():
            load(level + 1).wait()
            widen(level + 1)

        combine(level, groups - 1)
        for h in range(max(0, groups - LAG), groups - 1):
            finish(level, h)
        return carry

    pl.semaphore_wait(barrier, peers)
    lax.fori_loop(0, level_count, one_level, 0)
    finish(level_count - 1, groups - 1)

    lane = lax.broadcasted_iota(jnp.int32, (ss, LANES), 1)
    line = lax.broadcasted_iota(jnp.int32, (ss, LANES), 0)
    peak = jnp.full((1, LANES), LOW, jnp.float32)
    for h in range(groups):
        wait_times(level_count - 1, h)
        for g in range(sub):
            for k in range(pin_groups):
                value = times_ref[level_count, h, g * pin_groups + k]
                start = h * gscen + g * ss
                out_ref[start:start + ss, k * sp:(k + 1) * sp] = value
                top = jnp.max(value, axis=1, keepdims=True)
                shown = jnp.where(lane == line + start, top, jnp.float32(LOW))
                peak = jnp.maximum(peak, jnp.max(shown, axis=0, keepdims=True))

    peak_ref[col] = peak

    def peak_copy(other, slot):
        return pltpu.make_async_remote_copy(
            src_ref=peak_ref.at[col], dst_ref=peak_ref.at[slot],
            send_sem=peak_send.at[other], recv_sem=peak_recv.at[slot],
            device_id=(row, other), device_id_type=MESH)

    for n in range(1, cols):
        peak_copy(lax.rem(col + n, cols), col).start()

    def settle(level, carry):
        for h in range(groups):
            for n in range(1, ratio):
                pair_copy(level, h, lax.rem(p + n, ratio), p).wait_send()
            for n in range(1, slices):
                rs_copy(level, h, lax.rem(z + n, slices), z).wait_send()
            for n in range(1, rows):
                times_copy(level, h, lax.rem(row + n, rows), z).wait_send()

            @pl.when(row != z)
            def _():
                times_copy(level, h, row, z).wait_send()

        return carry

    lax.fori_loop(0, level_count, settle, 0)

    for n in range(1, cols):
        other = lax.rem(col + n, cols)
        peak_copy(other, other).wait_recv()
        peak = jnp.maximum(peak, peak_ref[other])
    worst_ref[...] = peak
    for n in range(1, cols):
        peak_copy(lax.rem(col + n, cols), col).wait_send()


def shards(arrival, delay, occupancy):
    rows, cols = lax.axis_size("row"), lax.axis_size("col")
    scenarios, tile = arrival.shape
    level_count, _, width = delay.shape
    ratio = cols // rows
    sp = LANES
    pin_groups = tile // sp
    sub = rows // pin_groups
    ss = max(8, 16 // sub)
    groups = scenarios // (sub * ss)
    vmem = pl.BlockSpec(memory_space=pltpu.VMEM)
    f32 = jnp.float32
    dma = pltpu.SemaphoreType.DMA
    times, worst = pl.pallas_call(
        functools.partial(kernel, rows, cols),
        out_shape=(
            jax.ShapeDtypeStruct((scenarios, tile), f32),
            jax.ShapeDtypeStruct((1, LANES), f32),
        ),
        in_specs=[vmem, pl.BlockSpec(memory_space=pltpu.HBM), pl.BlockSpec(memory_space=pltpu.SMEM)],
        out_specs=(vmem, vmem),
        scratch_shapes=[
            pltpu.VMEM((level_count, tile, width), delay.dtype),
            pltpu.VMEM((level_count, tile // 8, 8, width), f32),
            pltpu.VMEM((level_count, ratio, groups, rows, ss, sp), f32),
            pltpu.VMEM((level_count, ratio, groups, rows, ss, sp), f32),
            pltpu.VMEM((level_count, groups, rows, ss, sp), f32),
            pltpu.VMEM((level_count, groups, rows, ss, sp), f32),
            pltpu.VMEM((level_count, groups, ss, sp), f32),
            pltpu.VMEM((level_count + 1, groups, rows, ss, sp), f32),
            pltpu.VMEM((cols, 1, LANES), f32),
            dma((level_count,)),
            dma((level_count, groups, ratio)), dma((level_count, groups, ratio)),
            dma((level_count, groups, rows)), dma((level_count, groups, rows)),
            dma((level_count, groups, rows)), dma((level_count, groups, rows)),
            dma((cols,)), dma((cols,)),
        ],
        compiler_params=pltpu.CompilerParams(collective_id=0, has_side_effects=True, vmem_limit_bytes=60 * 1024 * 1024),
    )(arrival, delay, occupancy)
    return times, worst[0, :scenarios]


def solution(mesh):
    placed = (P(None, "col"), P(None, "col", "row"), P())
    return jax.shard_map(
        shards, mesh=mesh, in_specs=placed, out_specs=(P(None, "col"), P()), check_vma=False
    )
```

```python
import functools

import jax
import jax.numpy as jnp
from jax import lax
from jax.experimental import pallas as pl
from jax.experimental.pallas import tpu as pltpu
from jax.sharding import PartitionSpec as P

MESH = pl.DeviceIdType.MESH
LANES = 128
GROUP = 128
LAG = 3
LOW = -1000000000.0


def kernel(
    rows, cols, arrival_ref, delay_hbm, occ_ref, out_ref, worst_ref,
    delay_ref, wide_ref, part_ref, pair_ref, comb_ref, rs_ref, fin_ref, times_ref, peak_ref, top_ref,
    load_sem, pair_send, pair_recv, rs_send, rs_recv, times_send, times_recv, peak_send, peak_recv, top_send, top_recv,
):
    level_count, tile, width = delay_hbm.shape
    ratio = cols // rows
    groups, slices, ss, sp = times_ref.shape[1:]
    pin_groups = tile // sp
    sub = slices // pin_groups
    gscen = sub * ss
    row = lax.axis_index("row")
    col = lax.axis_index("col")
    z = col // ratio
    p = col % ratio

    barrier = pltpu.get_barrier_semaphore()

    def greet(to_row, to_col):
        pl.semaphore_signal(barrier, inc=1, device_id=(to_row, to_col), device_id_type=MESH)

    for n in range(1, cols):
        greet(row, lax.rem(col + n, cols))
    for n in range(1, rows):
        greet(lax.rem(row + n, rows), col)
        greet(lax.rem(row + n, rows), row * ratio + p)
        greet(z, lax.rem(z + n, slices) * ratio + p)

    @pl.when(row != z)
    def _():
        greet(row, row * ratio + p)
        greet(z, z * ratio + p)

    peers = cols - 1 + 3 * (rows - 1) + 2 * (row != z).astype(jnp.int32)

    def load(level):
        return pltpu.make_async_copy(delay_hbm.at[level], delay_ref.at[level], load_sem.at[level])

    for level in range(level_count):
        load(level).start()

    def widen(level):
        def step(i, carry):
            at = pl.ds(pl.multiple_of(i * 64, 64), 64)
            wide_ref[level, pl.ds(i * 8, 8)] = delay_ref[level, at, :].astype(jnp.float32).reshape(8, 8, width)
            return carry

        lax.fori_loop(0, tile // 64, step, 0)

    for h in range(groups):
        for g in range(sub):
            for k in range(pin_groups):
                start = h * gscen + g * ss
                times_ref[0, h, g * pin_groups + k] = arrival_ref[start:start + ss, k * sp:(k + 1) * sp]
    load(0).wait()
    widen(0)

    def compute(level, h, middle):
        def step(n, best):
            @pl.when(n == tile // GROUP // 2)
            def _():
                middle()

            k = n // (sp // GROUP)
            value = jnp.concatenate([times_ref[level, h, g * pin_groups + k] for g in range(sub)], axis=0)
            if GROUP < sp:
                value = pltpu.roll(value, sp - (n % (sp // GROUP)) * GROUP, 1)
            for i in range(GROUP):
                spread = jnp.broadcast_to(value[:, i:i + 1], (gscen, LANES))
                best = tuple(jnp.maximum(b, spread + wide_ref[level, n * (GROUP // 8) + i // 8, i % 8:i % 8 + 1, c * LANES:(c + 1) * LANES]) for c, b in enumerate(best))
            return best

        best = lax.fori_loop(0, tile // GROUP, step, (jnp.full((gscen, LANES), LOW, jnp.float32),) * (width // LANES))
        best = jnp.concatenate(best, axis=1)
        for q in range(ratio):
            flag = occ_ref[level, col, row * ratio + q]
            for g in range(sub):
                for k in range(pin_groups):
                    start = q * tile + k * sp
                    piece = best[g * ss:(g + 1) * ss, start:start + sp]
                    part_ref[level, q, h, g * pin_groups + k] = jnp.where(flag > 0, piece, jnp.float32(LOW))

    def pair_copy(level, h, q, slot):
        return pltpu.make_async_remote_copy(
            src_ref=part_ref.at[level, q, h], dst_ref=pair_ref.at[level, slot, h],
            send_sem=pair_send.at[level, h, q], recv_sem=pair_recv.at[level, h, slot],
            device_id=(row, z * ratio + q), device_id_type=MESH)

    def rs_copy(level, h, other, slot):
        return pltpu.make_async_remote_copy(
            src_ref=comb_ref.at[level, h, other], dst_ref=rs_ref.at[level, h, slot],
            send_sem=rs_send.at[level, h, other], recv_sem=rs_recv.at[level, h, slot],
            device_id=(row, other * ratio + p), device_id_type=MESH)

    def times_copy(level, h, to, slot):
        return pltpu.make_async_remote_copy(
            src_ref=fin_ref.at[level, h], dst_ref=times_ref.at[level + 1, h, slot],
            send_sem=times_send.at[level, h, to], recv_sem=times_recv.at[level, h, slot],
            device_id=(to, row * ratio + p), device_id_type=MESH)

    def wait_times(level, h):
        for n in range(1, slices):
            times_copy(level, h, 0, lax.rem(z + n, slices)).wait_recv()

        @pl.when(row != z)
        def _():
            times_copy(level, h, 0, z).wait_recv()

    def combine(level, h):
        total = part_ref[level, p, h]
        for n in range(1, ratio):
            q = lax.rem(p + n, ratio)
            pair_copy(level, h, q, q).wait_recv()
            total = jnp.maximum(total, pair_ref[level, q, h])
        comb_ref[level, h] = total
        for n in range(1, slices):
            rs_copy(level, h, lax.rem(z + n, slices), z).start()

    def finish(level, h):
        total = comb_ref[level, h, z]
        for n in range(1, slices):
            other = lax.rem(z + n, slices)
            rs_copy(level, h, other, other).wait_recv()
            total = jnp.maximum(total, rs_ref[level, h, other])
        fin_ref[level, h] = total
        for n in range(1, rows):
            times_copy(level, h, lax.rem(row + n, rows), z).start()

        @pl.when(row != z)
        def _():
            times_copy(level, h, row, z).start()

        @pl.when(row == z)
        def _():
            times_ref[level + 1, h, z] = fin_ref[level, h]

    def one_level(level, carry):
        for h in range(groups):
            @pl.when(level > 0)
            def _():
                wait_times(level - 1, h)

            def middle():
                if h >= 1:
                    combine(level, h - 1)
                else:
                    @pl.when(level > 0)
                    def _():
                        finish(level - 1, groups - 1)
                if h >= LAG:
                    finish(level, h - LAG)

            compute(level, h, middle)
            for n in range(1, ratio):
                pair_copy(level, h, lax.rem(p + n, ratio), p).start()

        @pl.when(level + 1 < level_count)
        def _():
            load(level + 1).wait()
            widen(level + 1)

        combine(level, groups - 1)
        for h in range(max(0, groups - LAG), groups - 1):
            finish(level, h)
        return carry

    pl.semaphore_wait(barrier, peers)
    lax.fori_loop(0, level_count, one_level, 0)
    finish(level_count - 1, groups - 1)

    lane = lax.broadcasted_iota(jnp.int32, (ss, LANES), 1)
    line = lax.broadcasted_iota(jnp.int32, (ss, LANES), 0)
    peak = jnp.full((1, LANES), LOW, jnp.float32)
    for h in range(groups):
        top = jnp.max(fin_ref[level_count - 1, h], axis=1, keepdims=True)
        shown = jnp.where(lane == line + h * gscen + z // pin_groups * ss, top, jnp.float32(LOW))
        peak = jnp.maximum(peak, jnp.max(shown, axis=0, keepdims=True))
    peak_ref[col] = peak

    def peak_copy(other, slot):
        return pltpu.make_async_remote_copy(
            src_ref=peak_ref.at[col], dst_ref=peak_ref.at[slot],
            send_sem=peak_send.at[other], recv_sem=peak_recv.at[slot],
            device_id=(row, other), device_id_type=MESH)

    def top_copy(other, slot):
        return pltpu.make_async_remote_copy(
            src_ref=top_ref.at[row], dst_ref=top_ref.at[slot],
            send_sem=top_send.at[other], recv_sem=top_recv.at[slot],
            device_id=(other, col), device_id_type=MESH)

    for n in range(1, cols):
        peak_copy(lax.rem(col + n, cols), col).start()
    for n in range(1, cols):
        other = lax.rem(col + n, cols)
        peak_copy(other, other).wait_recv()
        peak = jnp.maximum(peak, peak_ref[other])
    top_ref[row] = peak
    for n in range(1, rows):
        top_copy(lax.rem(row + n, rows), row).start()

    for h in range(groups):
        wait_times(level_count - 1, h)
        for g in range(sub):
            for k in range(pin_groups):
                start = h * gscen + g * ss
                out_ref[start:start + ss, k * sp:(k + 1) * sp] = times_ref[level_count, h, g * pin_groups + k]

    def settle(level, carry):
        for h in range(groups):
            for n in range(1, ratio):
                pair_copy(level, h, lax.rem(p + n, ratio), p).wait_send()
            for n in range(1, slices):
                rs_copy(level, h, lax.rem(z + n, slices), z).wait_send()
            for n in range(1, rows):
                times_copy(level, h, lax.rem(row + n, rows), z).wait_send()

            @pl.when(row != z)
            def _():
                times_copy(level, h, row, z).wait_send()

        return carry

    lax.fori_loop(0, level_count, settle, 0)

    for n in range(1, rows):
        other = lax.rem(row + n, rows)
        top_copy(other, other).wait_recv()
        peak = jnp.maximum(peak, top_ref[other])
    worst_ref[...] = peak
    for n in range(1, cols):
        peak_copy(lax.rem(col + n, cols), col).wait_send()
    for n in range(1, rows):
        top_copy(lax.rem(row + n, rows), row).wait_send()


def shards(arrival, delay, occupancy):
    rows, cols = lax.axis_size("row"), lax.axis_size("col")
    scenarios, tile = arrival.shape
    level_count, _, width = delay.shape
    ratio = cols // rows
    sp = LANES
    pin_groups = tile // sp
    sub = rows // pin_groups
    ss = max(8, 16 // sub)
    groups = scenarios // (sub * ss)
    vmem = pl.BlockSpec(memory_space=pltpu.VMEM)
    f32 = jnp.float32
    dma = pltpu.SemaphoreType.DMA
    times, worst = pl.pallas_call(
        functools.partial(kernel, rows, cols),
        out_shape=(
            jax.ShapeDtypeStruct((scenarios, tile), f32),
            jax.ShapeDtypeStruct((1, LANES), f32),
        ),
        in_specs=[vmem, pl.BlockSpec(memory_space=pltpu.HBM), pl.BlockSpec(memory_space=pltpu.SMEM)],
        out_specs=(vmem, vmem),
        scratch_shapes=[
            pltpu.VMEM((level_count, tile, width), delay.dtype),
            pltpu.VMEM((level_count, tile // 8, 8, width), f32),
            pltpu.VMEM((level_count, ratio, groups, rows, ss, sp), f32),
            pltpu.VMEM((level_count, ratio, groups, rows, ss, sp), f32),
            pltpu.VMEM((level_count, groups, rows, ss, sp), f32),
            pltpu.VMEM((level_count, groups, rows, ss, sp), f32),
            pltpu.VMEM((level_count, groups, ss, sp), f32),
            pltpu.VMEM((level_count + 1, groups, rows, ss, sp), f32),
            pltpu.VMEM((cols, 1, LANES), f32),
            pltpu.VMEM((rows, 1, LANES), f32),
            dma((level_count,)),
            dma((level_count, groups, ratio)), dma((level_count, groups, ratio)),
            dma((level_count, groups, rows)), dma((level_count, groups, rows)),
            dma((level_count, groups, rows)), dma((level_count, groups, rows)),
            dma((cols,)), dma((cols,)),
            dma((rows,)), dma((rows,)),
        ],
        compiler_params=pltpu.CompilerParams(collective_id=0, has_side_effects=True, vmem_limit_bytes=60 * 1024 * 1024),
    )(arrival, delay, occupancy)
    return times, worst[0, :scenarios]


def solution(mesh):
    placed = (P(None, "col"), P(None, "col", "row"), P())
    return jax.shard_map(
        shards, mesh=mesh, in_specs=placed, out_specs=(P(None, "col"), P()), check_vma=False
    )
```
